256 devices in a mesh: state: 8 (over z), act: 32 (over x, y, core).
Axes of the slice: x: 4, y: 4, z: 8, core: 2. Of those that a mesh axis runs over, the one named last changes fastest.
Arguments:
- state_features: bfloat16 [768, 2048], P('state', 'act'), may hold values from -6 to 6
- action_features: bfloat16 [768, 256, 2048], P('state', 'act'), may hold values from -240 to 240
- targets: float32 [768], P('state'), may hold values from -12 to 12
- w_hidden: bfloat16 [2048, 2048], replicated, may hold values from -0.125 to 0.125
- w_head: float32 [2048], replicated, may hold values from -7 to 7
Outputs:
- grad_hidden: float32 [2048, 2048], P(('state', 'act'))
- grad_head: float32 [2048], replicated
- log_partition: float32 [768], P('state')
- mean_loss: float32 [], replicated
The draws below stay inside these ranges and needn't reach their ends.
All inputs are finite; a program needn't handle non-finite values.
Results may differ from the reference program's by a relative error of at most 0.006.
Values may be sent and summed in bfloat16 or wider, within the bound.
No kernel may reach another device: no remote copies, remote signals or barrier semaphores. Data moves between devices by JAX's collectives and lax.ppermute only.
A program may use at most 128 MiB of HBM per device.

```python
import jax
import jax.numpy as jnp
from jax import lax

D = 2048
STATES = 768
ACTIONS = 256


def head_base(key):
    return jnp.clip(jax.random.normal(jax.random.fold_in(key, 7), (D,), jnp.float32), -6.0, 6.0)


def head_scale():
    return 150.0


def draw_w_head(key, part):
    base = head_base(key)
    return base * (head_scale() / D)


def draw_action_features(key, part):
    noise = jnp.clip(jax.random.normal(jax.random.fold_in(key, 11), (STATES, ACTIONS, D), jnp.float32), -6.0, 6.0)
    base = head_base(key)
    base_rms = jnp.sqrt(jnp.mean(base * base))
    direction = base / base_rms
    picked_states = jax.random.randint(jax.random.fold_in(key, 13), (6,), 0, STATES)
    picked_actions = jax.random.randint(jax.random.fold_in(key, 17), (6,), 0, ACTIONS - 1)
    strength = jnp.array([0.7, 0.8, 0.9, 0.7, 0.8, 0.9], jnp.float32)
    fresh = noise[picked_states, picked_actions]
    upper = 20.0 * (strength[:, None] * direction[None, :] + jnp.sqrt(1.0 - strength * strength)[:, None] * fresh) / 6.0 * 6.0
    lower_strength = strength - 2.0 / (head_scale() * base_rms)
    lower = 20.0 * (lower_strength[:, None] * direction[None, :] + jnp.sqrt(1.0 - lower_strength * lower_strength)[:, None] * fresh)
    noise = noise.at[picked_states, picked_actions].set(upper)
    noise = noise.at[picked_states, picked_actions + 1].set(lower)
    return noise.astype(jnp.bfloat16)


def block_scale(stream_key, shape, split, smallest, largest):
    def one(position, parts):
        steps = jax.random.uniform(jax.random.fold_in(jax.random.fold_in(stream_key, 6), position), (parts,), jnp.float32, smallest / len(split), largest / len(split))
        return jnp.repeat(jnp.exp(steps), shape[position] // parts).reshape((-1,) + (1,) * (len(shape) - position - 1))

    factor_of = one(*split[0])
    for cut in split[1:]:
        factor_of = factor_of * one(*cut)
    return factor_of


def scatter_about(key, shape, scale, bound, shards=(), kind=jnp.bfloat16):
    values = scale * jax.random.normal(key, shape, jnp.float32)
    if shards:
        values = values * block_scale(key, shape, shards, -0.22, 0.18)
    return jnp.clip(values, -bound, bound).astype(kind)


def setup_inputs(seed: int = 0) -> dict:
    arg_keys = jax.random.split(jax.random.key(seed), 6)
    return {
        "state_features": scatter_about(arg_keys[0], (STATES, D), 1.0, 6.0, ((0, 8), (1, 32))),
        "action_features": draw_action_features(jax.random.fold_in(arg_keys[5], 71), 0),
        "targets": scatter_about(arg_keys[2], (STATES,), 2.0, 12.0, ((0, 8),), jnp.float32),
        "w_hidden": scatter_about(arg_keys[3], (D, D), D ** -0.5, 0.125),
        "w_head": draw_w_head(jax.random.fold_in(arg_keys[5], 71), 0),
    }


norm_epsilon = 1e-06
penalty_weight = 2.0

def reference(state_features, action_features, targets, w_hidden, w_head):
    blocks = STATES // 8

    def block_step(partial_value, block_index):
        grad_hidden, grad_head, loss_sum = partial_value
        state_block = lax.dynamic_slice_in_dim(state_features, block_index * 8, 8, 0)
        action_block = lax.dynamic_slice_in_dim(action_features, block_index * 8, 8, 0)
        target_block = lax.dynamic_slice_in_dim(targets, block_index * 8, 8, 0)
        mixture = state_block.astype(jnp.float32)[:, None, :] + action_block.astype(jnp.float32)
        normed = (mixture * lax.rsqrt(lax.optimization_barrier(jnp.mean(mixture * mixture, -1, keepdims=True)) + norm_epsilon)).astype(jnp.bfloat16)
        flat_rows = normed.reshape(-1, D)
        preact = jnp.dot(flat_rows, w_hidden, preferred_element_type=jnp.float32)
        sigmoid_pre = jax.nn.sigmoid(preact)
        head_input = flat_rows.astype(jnp.float32) + preact * sigmoid_pre
        scores = lax.optimization_barrier(jnp.sum(head_input * w_head, -1)).reshape(8, ACTIONS)
        row_max = lax.optimization_barrier(jnp.max(scores, -1, keepdims=True))
        log_part = row_max[:, 0] + jnp.log(lax.optimization_barrier(jnp.sum(jnp.exp(scores - row_max), -1)))
        softmax_weight = jnp.exp(scores - log_part[:, None])
        is_data = (jnp.arange(ACTIONS, dtype=jnp.int32) == 0)[None, :]
        bellman_gap = scores - target_block[:, None]
        score_grad = penalty_weight * softmax_weight + jnp.where(is_data, bellman_gap - penalty_weight, 0.0)
        loss_terms = jnp.where(is_data, penalty_weight * (log_part[:, None] - scores) + 0.5 * bellman_gap * bellman_gap, 0.0)
        grad_flat = score_grad.reshape(-1)
        grad_head = grad_head + lax.optimization_barrier(jnp.sum(grad_flat[:, None] * head_input, 0))
        back_grad = (grad_flat[:, None] * w_head * (sigmoid_pre + preact * sigmoid_pre * (1.0 - sigmoid_pre))).astype(jnp.bfloat16)
        grad_hidden = grad_hidden + lax.dot_general(flat_rows, back_grad, (((0,), (0,)), ((), ())), preferred_element_type=jnp.float32)
        return ((grad_hidden, grad_head, loss_sum + jnp.sum(loss_terms)), log_part)
    initial = (jnp.zeros((D, D), jnp.float32), jnp.zeros((D,), jnp.float32), jnp.zeros((), jnp.float32))
    (grad_hidden, grad_head, loss_sum), log_parts = lax.scan(block_step, initial, jnp.arange(blocks, dtype=jnp.int32))
    return (grad_hidden, grad_head, log_parts.reshape(STATES), loss_sum / STATES)
```

```python
import functools

import jax
import jax.numpy as jnp
from jax import lax
from jax.experimental import pallas as pl
from jax.experimental.pallas import tpu as pltpu
from jax.sharding import Mesh
from jax.sharding import PartitionSpec as P

ACT = ("x", "y", "c")
EVERY = ("z", "x", "y", "c")
F32 = jnp.float32
BF16 = jnp.bfloat16

norm_epsilon = 1e-06
penalty_weight = 2.0


ROWS = 256
COLS = 256


def shifted(value, axis, step):
    count = lax.axis_size(axis)
    return lax.ppermute(value, axis, [(i, (i + step) % count) for i in range(count)])


def within(value, op):
    lane = lax.broadcasted_iota(jnp.int32, value.shape, 1)
    width = value.shape[1]
    for step in (1, 2, 4):
        low = pltpu.roll(value, step, 1)
        high = pltpu.roll(value, width - step, 1)
        value = op(value, jnp.where((lane & step) != 0, low, high))
    return value


def forward_kernel(core_ref, s_ref, a_ref, w_ref, head_ref, xt_ref, keep_ref, send_ref, h_ref, score_ref, stats_ref, x_ref, tally_ref):
    height, width = a_ref.shape
    tiles = width // COLS
    at = pl.program_id(0)

    def normalise(i, carry):
        row = pl.multiple_of(i * 16, 16)
        acts = a_ref[pl.ds(row, 16), :].astype(F32)
        first = jnp.broadcast_to(s_ref[pl.ds(2 * i, 1), :], (8, width))
        second = jnp.broadcast_to(s_ref[pl.ds(2 * i + 1, 1), :], (8, width))
        mixture = jnp.concatenate([first, second], 0) + acts
        scale = lax.rsqrt(jnp.mean(mixture * mixture, -1, keepdims=True) + norm_epsilon)
        x_ref[pl.ds(row, 16), :] = (mixture * scale).astype(BF16)
        return carry

    lax.fori_loop(0, height // 16, normalise, 0)
    core = core_ref[0]
    total = jnp.zeros((height, 128), F32)
    x = x_ref[...]
    for j in range(tiles):
        n = pl.multiple_of(lax.rem(j + core * (tiles // 2), tiles) * COLS, COLS)
        x_cols = x_ref[:, pl.ds(n, COLS)]
        xt_ref[pl.ds(n, COLS), :] = x_cols.T
        preact = jnp.dot(x, w_ref[:, pl.ds(n, COLS)], preferred_element_type=F32)
        g = jax.nn.sigmoid(preact)
        gated = preact * g
        h = x_cols.astype(F32) + gated
        head = head_ref[:, pl.ds(n, COLS)]
        h_ref[:, pl.ds(n, COLS)] = h.astype(BF16)
        u = (head * (g + gated * (1.0 - g))).astype(BF16)
        if j < tiles // 2:
            keep_ref[:, j * COLS : (j + 1) * COLS] = u
        else:
            send_ref[:, j * COLS - width // 2 : (j + 1) * COLS - width // 2] = u
        part = h * head
        for k in range(COLS // 128):
            total += part[:, k * 128 : (k + 1) * 128]
    score = jnp.sum(total.T, 0, keepdims=True)
    score_ref[...] = score
    score = jnp.broadcast_to(score, (8, height))
    peak = within(score, jnp.maximum)
    mass = within(jnp.exp(score - peak), jnp.add)
    pair = jnp.where(lax.broadcasted_iota(jnp.int32, score.shape, 0) == 0, peak, mass)
    row = lax.broadcasted_iota(jnp.int32, (height, 128), 0)
    lane = lax.broadcasted_iota(jnp.int32, (height, 128), 1)
    pick = (row == (lane - at * (height // 8)) * 8).astype(F32)
    packed = jnp.dot(pair, pick, precision=lax.Precision.HIGHEST, preferred_element_type=F32)

    @pl.when(at == 0)
    def _():
        tally_ref[...] = jnp.zeros_like(tally_ref)

    tally_ref[...] += packed
    stats_ref[...] = jnp.broadcast_to(tally_ref[0:2, :][None], stats_ref.shape)


def forward(core, states, acts, w_hidden, w_head, members):
    rows, width = acts.shape
    half = width // 2
    tile = lambda cols: pl.BlockSpec((ROWS, cols), lambda i, core: (i, 0))
    return pl.pallas_call(
        forward_kernel,
        grid_spec=pltpu.PrefetchScalarGridSpec(
            num_scalar_prefetch=1,
            grid=(rows // ROWS,),
            in_specs=[
                pl.BlockSpec((ROWS // 8, width), lambda i, core: (i, 0)),
                tile(width),
                pl.BlockSpec(memory_space=pltpu.VMEM),
                pl.BlockSpec((1, width), lambda i, core: (0, 0)),
            ],
            out_specs=[
                pl.BlockSpec((width, ROWS), lambda i, core: (0, i)),
                tile(half),
                tile(half),
                tile(width),
                pl.BlockSpec((1, ROWS), lambda i, core: (0, i)),
                pl.BlockSpec((members, 2, 128), lambda i, core: (0, 0, 0)),
            ],
            scratch_shapes=[pltpu.VMEM((ROWS, width), BF16), pltpu.VMEM((8, 128), F32)],
        ),
        out_shape=[
            jax.ShapeDtypeStruct((width, rows), BF16),
            jax.ShapeDtypeStruct((rows, half), BF16),
            jax.ShapeDtypeStruct((rows, half), BF16),
            jax.ShapeDtypeStruct((rows, width), BF16),
            jax.ShapeDtypeStruct((1, rows), F32),
            jax.ShapeDtypeStruct((members, 2, 128), F32),
        ],
        compiler_params=pltpu.CompilerParams(vmem_limit_bytes=30 << 20),
        cost_estimate=pl.CostEstimate(flops=2 * rows * width * width, bytes_accessed=20 << 20, transcendentals=2 * rows * width),
        name="forward",
    )(core, states, acts, w_hidden, w_head)


def split(value):
    high = value.astype(BF16)
    return high, (value - high.astype(F32)).astype(BF16)


def middle_kernel(states_here, first_ref, stats_ref, here_ref, there_ref, target_ref, keep_ref, came_ref, h_ref, bo_ref, bp_ref, extra_ref, log_ref, grad_ref):
    rows, half = keep_ref.shape
    peaks = stats_ref[:, 0, :]
    peak = jnp.max(peaks, 0, keepdims=True)
    mass = jnp.sum(stats_ref[:, 1, :] * jnp.exp(peaks - peak), 0, keepdims=True)
    lane = lax.broadcasted_iota(jnp.int32, (1, 128), 1)
    log_partition = jnp.where(lane < states_here, peak + jnp.log(jnp.where(lane < states_here, mass, 1.0)), 0.0)
    log_ref[...] = log_partition
    at = lax.broadcasted_iota(jnp.int32, (8, 128), 0)
    pair = jnp.where(at == 0, log_partition, target_ref[...])
    state = lax.broadcasted_iota(jnp.int32, (128, rows), 0)
    row = lax.broadcasted_iota(jnp.int32, (128, rows), 1)
    spread = ((row >> 3) == state).astype(F32)
    pair = jnp.dot(pair, spread, precision=lax.Precision.HIGHEST, preferred_element_type=F32)
    log_rows, target_rows = pair[0:1], pair[1:2]
    lead = (lax.broadcasted_iota(jnp.int32, (1, rows), 1) & 7) == 0

    def graded(score, flag):
        is_data = jnp.logical_and(lead, jnp.broadcast_to(flag, lead.shape) == 1)
        gap = score - target_rows
        grad = penalty_weight * jnp.exp(score - log_rows)
        grad = grad + jnp.where(is_data, gap - penalty_weight, 0.0)
        loss = jnp.where(is_data, penalty_weight * (log_rows - score) + 0.5 * gap * gap, 0.0)
        return grad, loss

    grad_here, loss = graded(here_ref[...], first_ref[0])
    grad_there, _ = graded(there_ref[...], first_ref[1])
    at = lax.broadcasted_iota(jnp.int32, (8, rows), 0)
    grads = jnp.where(at == 0, grad_here, grad_there)
    grad_ref[...] = grads.T
    loss = jnp.sum(loss, 1, keepdims=True)

    def scaled(i, carry):
        r = pl.ds(pl.multiple_of(i * 64, 64), 64)
        bo_ref[r, :] = (keep_ref[r, :].astype(F32) * grad_ref[r, 0:1]).astype(BF16)
        bp_ref[r, :] = (came_ref[r, :].astype(F32) * grad_ref[r, 1:2]).astype(BF16)
        return carry

    lax.fori_loop(0, rows // 64, scaled, 0)
    high, low = split(grad_here)
    weights = jnp.where(at == 0, high.astype(F32), low.astype(F32))
    weights = jnp.where(at < 2, weights, 0.0).astype(BF16)
    head = jnp.dot(weights, h_ref[...], preferred_element_type=F32)
    head = head[0:1] + head[1:2]
    loss = jnp.broadcast_to(loss, (1, half // 2))
    parts = [head[:, i * (half // 2) : (i + 1) * (half // 2)] for i in range(4)] + [loss]
    pack_extra(extra_ref, parts)


def pack_extra(ref, parts):
    at = lax.broadcasted_iota(jnp.int32, ref.shape, 0)
    out = jnp.zeros(ref.shape, F32)
    for i, part in enumerate(parts):
        high, low = split(part)
        out = jnp.where(at == i, high.astype(F32), out)
        out = jnp.where(at == i + 8, low.astype(F32), out)
    ref[...] = out.astype(BF16)


def middle(first, stats, here, there, targets, keep, came, h, states_here):
    rows, half = keep.shape
    whole = pl.BlockSpec(memory_space=pltpu.VMEM)
    return pl.pallas_call(
        functools.partial(middle_kernel, states_here),
        in_specs=[pl.BlockSpec(memory_space=pltpu.SMEM)] + [whole] * 7,
        out_specs=[whole] * 4,
        out_shape=[
            jax.ShapeDtypeStruct((rows, half), BF16),
            jax.ShapeDtypeStruct((rows, half), BF16),
            jax.ShapeDtypeStruct((16, half // 2), BF16),
            jax.ShapeDtypeStruct((1, 128), F32),
        ],
        scratch_shapes=[pltpu.VMEM((rows, 8), F32)],
        compiler_params=pltpu.CompilerParams(vmem_limit_bytes=8 << 20),
        cost_estimate=pl.CostEstimate(flops=1 << 30, bytes_accessed=9 << 20, transcendentals=0),
        name="middle",
    )(first, stats, here, there, targets, keep, came, h)


def gradient_kernel(spot_ref, xo_ref, xp_ref, bo_ref, bp_ref, extra_ref, ox_ref, oy_ref):
    depth = xo_ref.shape[-1]
    half = bo_ref.shape[1] // 2
    at_x = spot_ref[0]
    at_y = pl.multiple_of(spot_ref[1] * 16, 16)
    count = oy_ref.shape[0]

    def rows_x(ref):
        return ref[:, at_x, :, :].reshape(-1, depth)

    def rows_y(ref):
        return jnp.concatenate([ref[:, i, pl.ds(at_y, 16), :].reshape(-1, depth) for i in range(4)], 0)

    total = jnp.dot(rows_x(xo_ref), bo_ref[:, :half], preferred_element_type=F32)
    total += jnp.dot(rows_x(xp_ref), bp_ref[:, :half], preferred_element_type=F32)
    ox_ref[:count, :] = total.astype(BF16)
    ox_ref[count:, :] = extra_ref[...]
    total = jnp.dot(rows_y(xo_ref), bo_ref[:, half:], preferred_element_type=F32)
    total += jnp.dot(rows_y(xp_ref), bp_ref[:, half:], preferred_element_type=F32)
    oy_ref[...] = total.astype(BF16)


def gradient(spot, xo, xp, bo, bp, extra):
    depth = xo.shape[-1]
    half = bo.shape[1] // 2
    count = xo.shape[0] * xo.shape[2]
    whole = pl.BlockSpec(memory_space=pltpu.VMEM)
    return pl.pallas_call(
        gradient_kernel,
        in_specs=[pl.BlockSpec(memory_space=pltpu.SMEM)] + [whole] * 5,
        out_specs=[whole] * 2,
        out_shape=[jax.ShapeDtypeStruct((count + 16, half), BF16), jax.ShapeDtypeStruct((count, half), BF16)],
        compiler_params=pltpu.CompilerParams(vmem_limit_bytes=12 << 20),
        cost_estimate=pl.CostEstimate(flops=8 * count * half * depth, bytes_accessed=4 << 20, transcendentals=0),
        name="gradient",
    )(spot, xo, xp, bo, bp, extra)


def ordered_extra(scratch_ref, order_ref, values):
    for k, value in enumerate(values):
        scratch_ref[order_ref[k]] = value
    total = scratch_ref[0]
    for k in range(1, len(values)):
        total = total + scratch_ref[k]
    return total


def fold_kernel(lead, with_extra, spot_ref, *refs):
    own, got, outs = refs[0], refs[1:4], refs[4:8]
    rest = refs[8:]
    if lead:
        take = lambda ref, k: ref[pl.ds(pl.multiple_of(spot_ref[k] * 128, 128), 128), :].astype(F32)
    else:
        take = lambda ref, k: jnp.concatenate(
            [ref[pl.ds(pl.multiple_of(z * 64 + spot_ref[k] * 16, 16), 16), :] for z in range(8)], 0
        ).astype(F32)
    for k in (1, 2, 3, 0):
        value = take(own, k)
        for ref in got:
            value += take(ref, k)
        outs[k][:128, :] = value.astype(outs[k].dtype)
    if with_extra:
        whole = [ref[512:528, :].astype(F32) for ref in (own, *got)]
        total = ordered_extra(rest[0], spot_ref.at[pl.ds(4, 4)], [v[:8] + v[8:] for v in whole])
        high, low = split(total)
        block = jnp.concatenate([high.astype(F32), low.astype(F32)], 0)
        for k in range(4):
            outs[k][128:144, :] = block.astype(outs[k].dtype)


def fold(spot, own, got, lead, with_extra):
    whole = pl.BlockSpec(memory_space=pltpu.VMEM)
    height = 144 if with_extra else 128
    cols = own.shape[1]
    return pl.pallas_call(
        functools.partial(fold_kernel, lead, with_extra),
        in_specs=[pl.BlockSpec(memory_space=pltpu.SMEM)] + [whole] * 4,
        out_specs=[whole] * 4,
        out_shape=[jax.ShapeDtypeStruct((height, cols), F32 if k == 0 else BF16) for k in range(4)],
        scratch_shapes=[pltpu.VMEM((4, 8, cols), F32)] if with_extra else [],
        compiler_params=pltpu.CompilerParams(vmem_limit_bytes=6 << 20),
        cost_estimate=pl.CostEstimate(flops=1 << 20, bytes_accessed=3 << 20, transcendentals=0),
        name="fold",
    )(spot, own, *got)


def join_kernel(order_ref, *refs):
    ax, ay, out_ref, scratch_ref = refs[0:4], refs[4:8], refs[8], refs[9]
    half = ax[0].shape[1]
    whole = [ref[128:144, :].astype(F32) for ref in ax]
    total = ordered_extra(scratch_ref, order_ref, [v[:8] + v[8:] for v in whole])
    pieces = [total[i : i + 1, j * 128 : (j + 1) * 128] for i in range(5) for j in range(half // 128)]
    high, low = split(pieces[16])
    pieces[16:] = [high.astype(F32), low.astype(F32)]
    tail = []
    for k in range(3):
        at = lax.broadcasted_iota(jnp.int32, (8, 128), 0)
        block = jnp.zeros((8, 128), F32)
        for i, piece in enumerate(pieces[8 * k : 8 * k + 8]):
            block = jnp.where(at == i, piece, block)
        tail.append(block)
    tail = jnp.concatenate(tail, 1).astype(BF16)
    for z in range(8):
        for c in range(2):
            r = slice(z * 16 + c * 8, z * 16 + c * 8 + 8)
            sx = sum(ref[r, :].astype(F32) for ref in ax)
            sy = sum(ref[r, :].astype(F32) for ref in ay)
            out_ref[2 * z + c, :, :half] = sx.astype(BF16)
            out_ref[2 * z + c, :, half : 2 * half] = sy.astype(BF16)
            out_ref[2 * z + c, :, 2 * half :] = tail


def join(order, ax, ay):
    whole = pl.BlockSpec(memory_space=pltpu.VMEM)
    half = ax[0].shape[1]
    return pl.pallas_call(
        join_kernel,
        in_specs=[pl.BlockSpec(memory_space=pltpu.SMEM)] + [whole] * 8,
        out_specs=whole,
        out_shape=jax.ShapeDtypeStruct((16, 8, 2 * half + 384), BF16),
        scratch_shapes=[pltpu.VMEM((4, 8, half), F32)],
        compiler_params=pltpu.CompilerParams(vmem_limit_bytes=4 << 20),
        cost_estimate=pl.CostEstimate(flops=1 << 20, bytes_accessed=2 << 20, transcendentals=0),
        name="join",
    )(order, *ax, *ay)


def last_kernel(scale, all_ref, hidden_ref, head_ref, loss_ref):
    half = hidden_ref.shape[1] // 2
    for c in range(2):
        hidden_ref[:, c * half : (c + 1) * half] = sum(all_ref[2 * z + c, :, :half].astype(F32) for z in range(8))
    tail = sum(all_ref[i, :, half:].astype(F32) for i in range(16))
    head_ref[0:8, :] = tail[:, 0:128]
    head_ref[8:16, :] = tail[:, 128:256]
    loss_ref[...] = (tail[0:1, 256:384] + tail[1:2, 256:384]) * scale


def last(everything, states_total):
    whole = pl.BlockSpec(memory_space=pltpu.VMEM)
    width = 2 * (everything.shape[2] - 384)
    return pl.pallas_call(
        functools.partial(last_kernel, 1.0 / states_total),
        in_specs=[whole],
        out_specs=[whole] * 3,
        out_shape=[
            jax.ShapeDtypeStruct((8, width), F32),
            jax.ShapeDtypeStruct((16, 128), F32),
            jax.ShapeDtypeStruct((1, 128), F32),
        ],
        compiler_params=pltpu.CompilerParams(vmem_limit_bytes=4 << 20),
        name="last",
    )(everything)


def whole_states(state_features):
    own = jnp.broadcast_to(state_features, (16, *state_features.shape))
    mine = lax.all_to_all(own, ("x", "y"), split_axis=0, concat_axis=0, tiled=True)
    other = shifted(mine, "c", 1)
    c = lax.axis_index("c")
    both = jnp.stack([jnp.where(c == 0, mine, other), jnp.where(c == 0, other, mine)], 1)
    return jnp.moveaxis(both, 2, 0).reshape(state_features.shape[0], -1).astype(F32)


def step(state_features, action_features, targets, w_hidden, w_head):
    states_here, actions_here, width = action_features.shape
    states_total = states_here * lax.axis_size("z")
    rows = states_here * actions_here
    x, y, c = lax.axis_index("x"), lax.axis_index("y"), lax.axis_index("c")
    members = lax.axis_size(ACT)
    states = whole_states(state_features)
    core = jnp.full((1,), c, jnp.int32)
    xt, keep, send, h, score, stats = forward(core, states, action_features.reshape(rows, width), w_hidden, w_head[None], members)
    stats = lax.all_to_all(stats, ACT, split_axis=0, concat_axis=0, tiled=True)
    score_there = shifted(score, "c", 1)
    came = shifted(send, "c", 1)
    xt_there = shifted(xt, "c", 1)
    member = lax.axis_index(ACT)
    first = jnp.stack([member == 0, member + 1 - 2 * c == 0]).astype(jnp.int32)
    padded = jnp.pad(targets[None], ((0, 0), (0, 128 - states_here)))
    b_here, b_there, extra, log_row = middle(first, stats, score, score_there, padded, keep, came, h, states_here)

    xo = xt.reshape(8, 4, 64, rows)
    xp = xt_there.reshape(8, 4, 64, rows)

    def piece(k):
        spot = jnp.stack([lax.rem(x + k, 4), lax.rem(y + k, 4)]).astype(jnp.int32)
        return gradient(spot, xo, xp, b_here, b_there, extra)

    got_x, got_y = [], []
    for k in (2, 1, 3):
        out_x, out_y = piece(k)
        got_x.append(shifted(out_x, "x", k))
        got_y.append(shifted(out_y, "y", k))
    own_x, own_y = piece(0)

    spots = lambda at, far: jnp.stack([lax.rem(at + k, 4) for k in range(4)] + [lax.rem(far + k, 4) for k in (0, 2, 3, 1)]).astype(jnp.int32)
    fx = fold(spots(y, x), own_x, got_x, False, True)
    fy = fold(spots(x, y), own_y, got_y, True, False)
    more_x, more_y = [fx[0]], [fy[0]]
    for k in (1, 2, 3):
        more_x.append(shifted(fx[k], "y", k))
    for k in (1, 2, 3):
        more_y.append(shifted(fy[k], "x", k))
    order = jnp.stack([lax.rem(y + k, 4) for k in (0, 3, 2, 1)]).astype(jnp.int32)
    joined = join(order, more_x, more_y)
    everything = lax.all_to_all(joined, ("z", "c"), split_axis=0, concat_axis=0, tiled=True)
    hidden, head, loss = last(everything, states_total)
    return (hidden, head.reshape(-1), log_row[0, :states_here], loss[0, 0])


def solution(mesh):
    finer = Mesh(mesh.devices.reshape(mesh.shape["state"], 4, 4, 2), EVERY)
    placed = (P("z", ACT), P("z", ACT, None), P("z"), P(), P())
    return jax.shard_map(
        step,
        mesh=finer,
        in_specs=placed,
        out_specs=(P(EVERY, None), P(), P("z"), P()),
        check_vma=False,
    )
```

```python
import functools

import jax
import jax.numpy as jnp
from jax import lax
from jax.experimental import pallas as pl
from jax.experimental.pallas import tpu as pltpu
from jax.sharding import Mesh
from jax.sharding import PartitionSpec as P

ACT = ("x", "y", "c")
EVERY = ("z", "x", "y", "c")
F32 = jnp.float32
BF16 = jnp.bfloat16

norm_epsilon = 1e-06
penalty_weight = 2.0


COLS = 256
EARLY = 2


def shifted(value, axis, step):
    count = lax.axis_size(axis)
    return lax.ppermute(value, axis, [(i, (i + step) % count) for i in range(count)])


def within(value, op):
    lane = lax.broadcasted_iota(jnp.int32, value.shape, 1)
    width = value.shape[1]
    for step in (1, 2, 4):
        low = pltpu.roll(value, step, 1)
        high = pltpu.roll(value, width - step, 1)
        value = op(value, jnp.where((lane & step) != 0, low, high))
    return value


def forward_kernel(height, ids_ref, mine_ref, other_ref, a_hbm, w_hbm, head_hbm, xt_ref, keep_ref, send_ref, h_ref, score_ref, stats_ref, s_ref, x_ref, a_ref, w_ref, head_ref, a_sems, w_sems, head_sem):
    rows, width = a_hbm.shape
    tiles = width // COLS
    core = ids_ref[2]
    spots = [pl.multiple_of(lax.rem(j + core * (tiles // 2), tiles) * COLS, COLS) for j in range(tiles)]
    a_copies, w_copies = [], []
    for i in range(rows // height):
        part = pl.ds(i * height, height)
        a_copies.append(pltpu.make_async_copy(a_hbm.at[part], a_ref.at[part], a_sems.at[i]))
    for j in range(tiles):
        part = pl.ds(j * COLS, COLS)
        w_copies.append(pltpu.make_async_copy(w_hbm.at[part], w_ref.at[part], w_sems.at[j]))
    head_copy = pltpu.make_async_copy(head_hbm, head_ref, head_sem)
    for copy in (*a_copies[:EARLY], *w_copies, *a_copies[EARLY:], head_copy):
        copy.start()
    lead = jnp.broadcast_to(core == 0, mine_ref.shape[1:])
    for i in range(mine_ref.shape[0]):
        mine, other = mine_ref[i].astype(F32), other_ref[i].astype(F32)
        pair = jnp.concatenate([jnp.where(lead, mine, other), jnp.where(lead, other, mine)], 0)
        s_ref[:, i * 128 : (i + 1) * 128] = pair.T

    def normalise(row):
        r = slice(row, row + 16)
        acts = a_ref[r, :].astype(F32)
        at = row // 8
        first = jnp.broadcast_to(s_ref[at : at + 1, :], (8, width))
        second = jnp.broadcast_to(s_ref[at + 1 : at + 2, :], (8, width))
        mixture = jnp.concatenate([first, second], 0) + acts
        scale = lax.rsqrt(jnp.mean(mixture * mixture, -1, keepdims=True) + norm_epsilon)
        x_ref[r, :] = (mixture * scale).astype(BF16)

    for i in range(EARLY):
        a_copies[i].wait()
        for row in range(i * height, (i + 1) * height, 16):
            normalise(row)
    for copy in (*w_copies, *a_copies[EARLY:], head_copy):
        copy.wait()
    tally = jnp.zeros((8, 128), F32)
    ahead = height // 16 // tiles
    for at in range(rows // height):
        r = slice(at * height, (at + 1) * height)
        total = jnp.zeros((height, 128), F32)
        for j in range(tiles):
            n = spots[j]
            x_cols = x_ref[r, pl.ds(n, COLS)]
            xt_ref[pl.ds(n, COLS), r] = x_cols.T
            preact = jnp.dot(x_ref[r, :], w_ref[:, pl.ds(n, COLS)], preferred_element_type=F32)
            if at + EARLY < rows // height:
                for i in range(ahead):
                    normalise((at + EARLY) * height + (j * ahead + i) * 16)
            g = jax.nn.sigmoid(preact)
            gated = preact * g
            h = x_cols.astype(F32) + gated
            head = head_ref[:, pl.ds(n, COLS)]
            h_ref[r, pl.ds(n, COLS)] = h.astype(BF16)
            u = (head * (g + gated * (1.0 - g))).astype(BF16)
            if j < tiles // 2:
                keep_ref[r, j * COLS : (j + 1) * COLS] = u
            else:
                send_ref[r, j * COLS - width // 2 : (j + 1) * COLS - width // 2] = u
            part = h * head
            for k in range(COLS // 128):
                total += part[:, k * 128 : (k + 1) * 128]
        score = jnp.sum(total.T, 0, keepdims=True)
        score_ref[:, r] = score
        score = jnp.broadcast_to(score, (8, height))
        peak = within(score, jnp.maximum)
        mass = within(jnp.exp(score - peak), jnp.add)
        pair = jnp.where(lax.broadcasted_iota(jnp.int32, score.shape, 0) == 0, peak, mass)
        row = lax.broadcasted_iota(jnp.int32, (height, 128), 0)
        lane = lax.broadcasted_iota(jnp.int32, (height, 128), 1)
        pick = (row == (lane - at * (height // 8)) * 8).astype(F32)
        tally = tally + jnp.dot(pair, pick, precision=lax.Precision.HIGHEST, preferred_element_type=F32)
    at = lax.broadcasted_iota(jnp.int32, (8, 128), 0)
    payload = tally
    for k in range(rows // 128):
        payload = jnp.where(at == k + 2, score_ref[:, k * 128 : (k + 1) * 128], payload)
    stats_ref[...] = jnp.broadcast_to(payload[None], stats_ref.shape)


def forward(ids, mine, other, acts, w_hidden, w_head, members, height=256):
    rows, width = acts.shape
    half = width // 2
    whole = pl.BlockSpec(memory_space=pltpu.VMEM)
    away = pl.BlockSpec(memory_space=pltpu.HBM)
    acts = pltpu.with_memory_space_constraint(acts, pltpu.HBM)
    w_hidden = pltpu.with_memory_space_constraint(w_hidden, pltpu.HBM)
    w_head = pltpu.with_memory_space_constraint(w_head, pltpu.HBM)
    return pl.pallas_call(
        functools.partial(forward_kernel, height),
        in_specs=[pl.BlockSpec(memory_space=pltpu.SMEM), whole, whole, away, away, away],
        out_specs=[whole] * 6,
        out_shape=[
            jax.ShapeDtypeStruct((width, rows), BF16),
            jax.ShapeDtypeStruct((rows, half), BF16),
            jax.ShapeDtypeStruct((rows, half), BF16),
            jax.ShapeDtypeStruct((rows, width), BF16),
            jax.ShapeDtypeStruct((1, rows), F32),
            jax.ShapeDtypeStruct((members, 8, 128), F32),
        ],
        scratch_shapes=[
            pltpu.VMEM((rows // 8, width), F32),
            pltpu.VMEM((rows, width), BF16),
            pltpu.VMEM((rows, width), BF16),
            pltpu.VMEM((width, width), BF16),
            pltpu.VMEM((1, width), F32),
            pltpu.SemaphoreType.DMA((rows // height,)),
            pltpu.SemaphoreType.DMA((width // COLS,)),
            pltpu.SemaphoreType.DMA,
        ],
        compiler_params=pltpu.CompilerParams(vmem_limit_bytes=24 << 20),
        cost_estimate=pl.CostEstimate(flops=2 * rows * width * width, bytes_accessed=20 << 20, transcendentals=2 * rows * width),
        name="forward",
    )(ids, mine, other, acts, w_hidden, w_head)


def split(value):
    high = value.astype(BF16)
    return high, (value - high.astype(F32)).astype(BF16)


def middle_kernel(states_here, ids_ref, stats_ref, here_ref, target_ref, keep_ref, came_ref, h_ref, bo_ref, bp_ref, extra_ref, log_ref, grad_ref):
    rows, half = keep_ref.shape
    peaks = stats_ref[:, 0, :]
    peak = jnp.max(peaks, 0, keepdims=True)
    mass = jnp.sum(stats_ref[:, 1, :] * jnp.exp(peaks - peak), 0, keepdims=True)
    lane = lax.broadcasted_iota(jnp.int32, (1, 128), 1)
    log_partition = jnp.where(lane < states_here, peak + jnp.log(jnp.where(lane < states_here, mass, 1.0)), 0.0)
    log_ref[...] = log_partition
    at = lax.broadcasted_iota(jnp.int32, (8, 128), 0)
    pair = jnp.where(at == 0, log_partition, 0.0)
    state = lax.broadcasted_iota(jnp.int32, (128, rows), 0)
    row = lax.broadcasted_iota(jnp.int32, (128, rows), 1)
    spread = ((row >> 3) == state).astype(F32)
    pair = jnp.dot(pair, spread, precision=lax.Precision.HIGHEST, preferred_element_type=F32)
    log_rows = pair[0:1]
    goals = jnp.broadcast_to(target_ref[...], (8, states_here))
    target_rows = jnp.dot(goals, spread[:states_here], precision=lax.Precision.HIGHEST, preferred_element_type=F32)[0:1]
    member = ids_ref[0] * 8 + ids_ref[1] * 2 + ids_ref[2]
    lead = (lax.broadcasted_iota(jnp.int32, (1, rows), 1) & 7) == 0

    def graded(score, flag):
        is_data = jnp.logical_and(lead, jnp.broadcast_to(flag, lead.shape))
        gap = score - target_rows
        grad = penalty_weight * jnp.exp(score - log_rows)
        grad = grad + jnp.where(is_data, gap - penalty_weight, 0.0)
        loss = jnp.where(is_data, penalty_weight * (log_rows - score) + 0.5 * gap * gap, 0.0)
        return grad, loss

    grad_here, loss = graded(here_ref[...], member == 0)
    partner = ids_ref[0] * 8 + ids_ref[1] * 2 + 1 - ids_ref[2]
    sent = stats_ref[partner]
    there = jnp.concatenate([sent[k + 2 : k + 3] for k in range(rows // 128)], 1)
    grad_there, _ = graded(there, member + 1 - 2 * ids_ref[2] == 0)
    at = lax.broadcasted_iota(jnp.int32, (8, rows), 0)
    grads = jnp.where(at == 0, grad_here, grad_there)
    grad_ref[...] = grads.T
    loss = jnp.sum(loss, 1, keepdims=True)

    def scaled(i, carry):
        r = pl.ds(pl.multiple_of(i * 64, 64), 64)
        bo_ref[r, :] = (keep_ref[r, :].astype(F32) * grad_ref[r, 0:1]).astype(BF16)
        bp_ref[r, :] = (came_ref[r, :].astype(F32) * grad_ref[r, 1:2]).astype(BF16)
        return carry

    lax.fori_loop(0, rows // 64, scaled, 0)
    high, low = split(grad_here)
    weights = jnp.where(at == 0, high.astype(F32), low.astype(F32))
    weights = jnp.where(at < 2, weights, 0.0).astype(BF16)
    head = jnp.dot(weights, h_ref[...], preferred_element_type=F32)
    head = head[0:1] + head[1:2]
    pack_extra(extra_ref, [head[:, :half], head[:, half:], jnp.broadcast_to(loss, (1, half))])


def pack_extra(ref, parts):
    at = lax.broadcasted_iota(jnp.int32, ref.shape, 0)
    out = jnp.zeros(ref.shape, F32)
    for i, part in enumerate(parts):
        high, low = split(part)
        out = jnp.where(at == i, high.astype(F32), out)
        out = jnp.where(at == i + 8, low.astype(F32), out)
    ref[...] = out.astype(BF16)


def middle(ids, stats, here, targets, keep, came, h, states_here):
    rows, half = keep.shape
    whole = pl.BlockSpec(memory_space=pltpu.VMEM)
    return pl.pallas_call(
        functools.partial(middle_kernel, states_here),
        in_specs=[pl.BlockSpec(memory_space=pltpu.SMEM)] + [whole] * 6,
        out_specs=[whole] * 4,
        out_shape=[
            jax.ShapeDtypeStruct((rows, half), BF16),
            jax.ShapeDtypeStruct((rows, half), BF16),
            jax.ShapeDtypeStruct((16, half), BF16),
            jax.ShapeDtypeStruct((1, 128), F32),
        ],
        scratch_shapes=[pltpu.VMEM((rows, 8), F32)],
        compiler_params=pltpu.CompilerParams(vmem_limit_bytes=6 << 20),
        cost_estimate=pl.CostEstimate(flops=1 << 30, bytes_accessed=9 << 20, transcendentals=0),
        name="middle",
    )(ids, stats, here, targets, keep, came, h)


def ways(ids_ref):
    x, y, core = ids_ref[0], ids_ref[1], ids_ref[2]
    return jnp.where(core == 0, x, y), jnp.where(core == 0, y, x), core


def gradient_kernel(turn, ids_ref, xo_ref, xp_ref, bo_ref, bp_ref, extra_ref, out_ref):
    near, _, core = ways(ids_ref)
    at = lax.rem(near + turn, 4)
    base = at * jnp.where(core == 0, 64, 16)
    stride = jnp.where(core == 0, 16, 64)
    count = out_ref.shape[0] - 16

    def rows(ref):
        starts = [pl.multiple_of(z * 256 + base + i * stride, 16) for z in range(8) for i in range(4)]
        return jnp.concatenate([ref[pl.ds(start, 16), :] for start in starts], 0)

    total = jnp.dot(rows(xo_ref), bo_ref[...], preferred_element_type=F32)
    total += jnp.dot(rows(xp_ref), bp_ref[...], preferred_element_type=F32)
    out_ref[:count, :] = total.astype(BF16)
    out_ref[count:, :] = extra_ref[...]


def gradient(turn, ids, xo, xp, bo, bp, extra):
    width, depth = xo.shape
    half = bo.shape[1]
    count = width // 4
    whole = pl.BlockSpec(memory_space=pltpu.VMEM)
    return pl.pallas_call(
        functools.partial(gradient_kernel, turn),
        in_specs=[pl.BlockSpec(memory_space=pltpu.SMEM)] + [whole] * 5,
        out_specs=whole,
        out_shape=jax.ShapeDtypeStruct((count + 16, half), BF16),
        compiler_params=pltpu.CompilerParams(vmem_limit_bytes=12 << 20),
        cost_estimate=pl.CostEstimate(flops=4 * count * half * depth, bytes_accessed=4 << 20, transcendentals=0),
        name="gradient",
    )(ids, xo, xp, bo, bp, extra)


def ordered_extra(scratch_ref, order, values):
    for k, value in enumerate(values):
        scratch_ref[order[k]] = value
    total = scratch_ref[0]
    for k in range(1, len(values)):
        total = total + scratch_ref[k]
    return total


def fold_kernel(ids_ref, *refs):
    own, got, outs, scratch_ref = refs[0], refs[1:4], refs[4:8], refs[8]
    near, far, _ = ways(ids_ref)
    for k in (1, 2, 3, 0):
        spot = lax.rem(far + k, 4) * 16
        for z in range(8):
            r = pl.ds(pl.multiple_of(z * 64 + spot, 16), 16)
            value = own[r, :].astype(F32)
            for ref in got:
                value += ref[r, :].astype(F32)
            outs[k][z * 16 : z * 16 + 16, :] = value.astype(outs[k].dtype)
    whole = [ref[512:528, :].astype(F32) for ref in (own, *got)]
    total = ordered_extra(scratch_ref, [lax.rem(near + k, 4) for k in (0, 2, 3, 1)], [v[:8] + v[8:] for v in whole])
    high, low = split(total)
    block = jnp.concatenate([high.astype(F32), low.astype(F32)], 0)
    for k in range(4):
        outs[k][128:144, :] = block.astype(outs[k].dtype)


def fold(ids, own, got):
    whole = pl.BlockSpec(memory_space=pltpu.VMEM)
    cols = own.shape[1]
    return pl.pallas_call(
        fold_kernel,
        in_specs=[pl.BlockSpec(memory_space=pltpu.SMEM)] + [whole] * 4,
        out_specs=[whole] * 4,
        out_shape=[jax.ShapeDtypeStruct((144, cols), F32 if k == 0 else BF16) for k in range(4)],
        scratch_shapes=[pltpu.VMEM((4, 8, cols), F32)],
        compiler_params=pltpu.CompilerParams(vmem_limit_bytes=6 << 20),
        cost_estimate=pl.CostEstimate(flops=1 << 20, bytes_accessed=3 << 20, transcendentals=0),
        name="fold",
    )(ids, own, *got)


def join_kernel(ids_ref, *refs):
    got, out_ref, scratch_ref = refs[0:4], refs[4], refs[5]
    half = got[0].shape[1]
    _, far, _ = ways(ids_ref)
    whole = [ref[128:144, :].astype(F32) for ref in got]
    total = ordered_extra(scratch_ref, [lax.rem(far + k, 4) for k in (0, 3, 2, 1)], [v[:8] + v[8:] for v in whole])
    pieces = [total[i : i + 1, j * 128 : (j + 1) * 128] for i in range(2) for j in range(half // 128)]
    pieces += [part.astype(F32) for part in split(total[2:3, :128])]
    tail = []
    for k in range(3):
        at = lax.broadcasted_iota(jnp.int32, (8, 128), 0)
        block = jnp.zeros((8, 128), F32)
        for i, piece in enumerate(pieces[8 * k : 8 * k + 8]):
            block = jnp.where(at == i, piece, block)
        tail.append(block)
    tail = jnp.concatenate(tail, 1).astype(BF16)
    for i in range(16):
        out_ref[i, :, :half] = sum(ref[i * 8 : i * 8 + 8, :].astype(F32) for ref in got).astype(BF16)
        out_ref[i, :, half:] = tail


def join(ids, got):
    whole = pl.BlockSpec(memory_space=pltpu.VMEM)
    half = got[0].shape[1]
    return pl.pallas_call(
        join_kernel,
        in_specs=[pl.BlockSpec(memory_space=pltpu.SMEM)] + [whole] * 4,
        out_specs=whole,
        out_shape=jax.ShapeDtypeStruct((16, 8, half + 384), BF16),
        scratch_shapes=[pltpu.VMEM((4, 8, half), F32)],
        compiler_params=pltpu.CompilerParams(vmem_limit_bytes=4 << 20),
        cost_estimate=pl.CostEstimate(flops=1 << 20, bytes_accessed=2 << 20, transcendentals=0),
        name="join",
    )(ids, *got)


def last_kernel(scale, all_ref, hidden_ref, head_ref, loss_ref):
    half = hidden_ref.shape[1] // 2
    for c in range(2):
        hidden_ref[:, c * half : (c + 1) * half] = sum(all_ref[2 * z + c, :, :half].astype(F32) for z in range(8))
    tail = sum(all_ref[i, :, half:].astype(F32) for i in range(16))
    head_ref[0:8, :] = tail[:, 0:128]
    head_ref[8:16, :] = tail[:, 128:256]
    loss_ref[...] = (tail[0:1, 256:384] + tail[1:2, 256:384]) * scale


def last(everything, states_total):
    whole = pl.BlockSpec(memory_space=pltpu.VMEM)
    width = 2 * (everything.shape[2] - 384)
    return pl.pallas_call(
        functools.partial(last_kernel, 1.0 / states_total),
        in_specs=[whole],
        out_specs=[whole] * 3,
        out_shape=[
            jax.ShapeDtypeStruct((8, width), F32),
            jax.ShapeDtypeStruct((16, 128), F32),
            jax.ShapeDtypeStruct((1, 128), F32),
        ],
        compiler_params=pltpu.CompilerParams(vmem_limit_bytes=4 << 20),
        name="last",
    )(everything)


def gathered(state_features, ids):
    own = jnp.where(jnp.sum(ids) < 0, jnp.zeros_like(state_features), state_features)
    own = jnp.broadcast_to(own.T, (16, *state_features.shape[::-1]))
    mine = lax.all_to_all(own, ("x", "y"), split_axis=0, concat_axis=0, tiled=True)
    return mine, shifted(mine, "c", 1)


def step(state_features, action_features, targets, w_hidden, w_head):
    states_here, actions_here, width = action_features.shape
    states_total = states_here * lax.axis_size("z")
    rows = states_here * actions_here
    ids = jnp.stack([lax.axis_index(axis) for axis in (*ACT, "z")]).astype(jnp.int32)
    members = lax.axis_size(ACT)
    mine, other = gathered(state_features, ids)
    xt, keep, send, h, score, stats = forward(
        ids, mine, other, action_features.reshape(rows, width), w_hidden, w_head[None], members
    )
    stats = lax.all_to_all(stats, ACT, split_axis=0, concat_axis=0, tiled=True)
    came = shifted(send, "c", 1)
    xt_there = shifted(xt, "c", 1)
    b_here, b_there, extra, log_row = middle(ids, stats, score, targets[None], keep, came, h, states_here)

    def piece(k):
        return gradient(k, ids, xt, xt_there, b_here, b_there, extra)

    def turned(value, k, swap):
        pairs = []
        for i in range(32):
            px, py, pc = i // 8, i // 2 % 4, i % 2
            along_x = (pc == 0) != swap
            to = (px + k) % 4 * 8 + py * 2 + pc if along_x else px * 8 + (py + k) % 4 * 2 + pc
            pairs.append((i, to))
        return lax.ppermute(value, ACT, pairs)

    got = []
    for k in (2, 1, 3):
        out = piece(k)
        got.append(turned(out, k, False))
    folded = fold(ids, piece(0), got)
    more = [folded[0]]
    for k in (1, 2, 3):
        more.append(turned(folded[k], k, True))
    joined = join(ids, more)
    everything = lax.all_to_all(joined, ("z", "c"), split_axis=0, concat_axis=0, tiled=True)
    hidden, head, loss = last(everything, states_total)
    return (hidden, head.reshape(-1), log_row[0, :states_here], loss[0, 0])


def solution(mesh):
    finer = Mesh(mesh.devices.reshape(mesh.shape["state"], 4, 4, 2), EVERY)
    placed = (P("z", ACT), P("z", ACT, None), P("z"), P(), P())
    return jax.shard_map(
        step,
        mesh=finer,
        in_specs=placed,
        out_specs=(P(EVERY, None), P(), P("z"), P()),
        check_vma=False,
    )
```

```python
import functools

import jax
import jax.numpy as jnp
from jax import lax
from jax.experimental import pallas as pl
from jax.experimental.pallas import tpu as pltpu
from jax.sharding import Mesh
from jax.sharding import PartitionSpec as P

ACT = ("x", "y", "c")
EVERY = ("z", "x", "y", "c")
F32 = jnp.float32
BF16 = jnp.bfloat16

norm_epsilon = 1e-06
penalty_weight = 2.0


COLS = 256
EARLY = 1


def shifted(value, axis, step):
    count = lax.axis_size(axis)
    return lax.ppermute(value, axis, [(i, (i + step) % count) for i in range(count)])


def within(value, op):
    lane = lax.broadcasted_iota(jnp.int32, value.shape, 1)
    width = value.shape[1]
    for step in (1, 2, 4):
        low = pltpu.roll(value, step, 1)
        high = pltpu.roll(value, width - step, 1)
        value = op(value, jnp.where((lane & step) != 0, low, high))
    return value


def forward_kernel(height, ids_ref, mine_ref, other_ref, a_hbm, w_hbm, head_hbm, xt_ref, keep_ref, send_ref, h_ref, score_ref, stats_ref, s_ref, x_ref, a_ref, w_ref, head_ref, a_sems, w_sems, head_sem):
    rows, width = a_hbm.shape
    tiles = width // COLS
    core = ids_ref[2]
    spots = [pl.multiple_of(lax.rem(j + core * (tiles // 2), tiles) * COLS, COLS) for j in range(tiles)]
    a_copies, w_copies = [], []
    for i in range(rows // height):
        part = pl.ds(i * height, height)
        a_copies.append(pltpu.make_async_copy(a_hbm.at[part], a_ref.at[part], a_sems.at[i]))
    for j in range(tiles):
        part = pl.ds(j * COLS, COLS)
        w_copies.append(pltpu.make_async_copy(w_hbm.at[part], w_ref.at[part], w_sems.at[j]))
    head_copy = pltpu.make_async_copy(head_hbm, head_ref, head_sem)
    for copy in (*a_copies[:EARLY], *w_copies, *a_copies[EARLY:], head_copy):
        copy.start()
    lead = jnp.broadcast_to(core == 0, mine_ref.shape[1:])
    for i in range(mine_ref.shape[0]):
        mine, other = mine_ref[i].astype(F32), other_ref[i].astype(F32)
        pair = jnp.concatenate([jnp.where(lead, mine, other), jnp.where(lead, other, mine)], 0)
        s_ref[:, i * 128 : (i + 1) * 128] = pair.T

    def normalise(row):
        r = slice(row, row + 16)
        acts = a_ref[r, :].astype(F32)
        at = row // 8
        first = jnp.broadcast_to(s_ref[at : at + 1, :], (8, width))
        second = jnp.broadcast_to(s_ref[at + 1 : at + 2, :], (8, width))
        mixture = jnp.concatenate([first, second], 0) + acts
        scale = lax.rsqrt(jnp.mean(mixture * mixture, -1, keepdims=True) + norm_epsilon)
        x_ref[r, :] = (mixture * scale).astype(BF16)

    for i in range(EARLY):
        a_copies[i].wait()
        for row in range(i * height, (i + 1) * height, 16):
            normalise(row)
    for copy in (*w_copies, *a_copies[EARLY:], head_copy):
        copy.wait()
    tally = jnp.zeros((8, 128), F32)
    ahead = height // 16 // tiles
    for at in range(rows // height):
        r = slice(at * height, (at + 1) * height)
        total = jnp.zeros((height, 128), F32)
        for j in range(tiles):
            n = spots[j]
            x_cols = x_ref[r, pl.ds(n, COLS)]
            xt_ref[pl.ds(n, COLS), r] = x_cols.T
            preact = jnp.dot(x_ref[r, :], w_ref[:, pl.ds(n, COLS)], preferred_element_type=F32)
            if at + EARLY < rows // height:
                for i in range(ahead):
                    normalise((at + EARLY) * height + (j * ahead + i) * 16)
            g = jax.nn.sigmoid(preact)
            gated = preact * g
            h = x_cols.astype(F32) + gated
            head = head_ref[:, pl.ds(n, COLS)]
            h_ref[r, pl.ds(n, COLS)] = h.astype(BF16)
            u = (head * (g + gated * (1.0 - g))).astype(BF16)
            if j < tiles // 2:
                keep_ref[r, j * COLS : (j + 1) * COLS] = u
            else:
                send_ref[r, j * COLS - width // 2 : (j + 1) * COLS - width // 2] = u
            part = h * head
            for k in range(COLS // 128):
                total += part[:, k * 128 : (k + 1) * 128]
        score = jnp.sum(total.T, 0, keepdims=True)
        score_ref[:, r] = score
        score = jnp.broadcast_to(score, (8, height))
        peak = within(score, jnp.maximum)
        mass = within(jnp.exp(score - peak), jnp.add)
        pair = jnp.where(lax.broadcasted_iota(jnp.int32, score.shape, 0) == 0, peak, mass)
        row = lax.broadcasted_iota(jnp.int32, (height, 128), 0)
        lane = lax.broadcasted_iota(jnp.int32, (height, 128), 1)
        pick = (row == (lane - at * (height // 8)) * 8).astype(F32)
        tally = tally + jnp.dot(pair, pick, precision=lax.Precision.HIGHEST, preferred_element_type=F32)
    at = lax.broadcasted_iota(jnp.int32, (8, 128), 0)
    payload = tally
    for k in range(rows // 128):
        payload = jnp.where(at == k + 2, score_ref[:, k * 128 : (k + 1) * 128], payload)
    stats_ref[...] = jnp.broadcast_to(payload[None], stats_ref.shape)


def forward(ids, mine, other, acts, w_hidden, w_head, members, height=768):
    rows, width = acts.shape
    half = width // 2
    whole = pl.BlockSpec(memory_space=pltpu.VMEM)
    away = pl.BlockSpec(memory_space=pltpu.HBM)
    acts = pltpu.with_memory_space_constraint(acts, pltpu.HBM)
    w_hidden = pltpu.with_memory_space_constraint(w_hidden, pltpu.HBM)
    w_head = pltpu.with_memory_space_constraint(w_head, pltpu.HBM)
    return pl.pallas_call(
        functools.partial(forward_kernel, height),
        in_specs=[pl.BlockSpec(memory_space=pltpu.SMEM), whole, whole, away, away, away],
        out_specs=[whole] * 6,
        out_shape=[
            jax.ShapeDtypeStruct((width, rows), BF16),
            jax.ShapeDtypeStruct((rows, half), BF16),
            jax.ShapeDtypeStruct((rows, half), BF16),
            jax.ShapeDtypeStruct((rows, width), BF16),
            jax.ShapeDtypeStruct((1, rows), F32),
            jax.ShapeDtypeStruct((members, 8, 128), F32),
        ],
        scratch_shapes=[
            pltpu.VMEM((rows // 8, width), F32),
            pltpu.VMEM((rows, width), BF16),
            pltpu.VMEM((rows, width), BF16),
            pltpu.VMEM((width, width), BF16),
            pltpu.VMEM((1, width), F32),
            pltpu.SemaphoreType.DMA((rows // height,)),
            pltpu.SemaphoreType.DMA((width // COLS,)),
            pltpu.SemaphoreType.DMA,
        ],
        compiler_params=pltpu.CompilerParams(vmem_limit_bytes=24 << 20),
        cost_estimate=pl.CostEstimate(flops=2 * rows * width * width, bytes_accessed=20 << 20, transcendentals=2 * rows * width),
        name="forward",
    )(ids, mine, other, acts, w_hidden, w_head)


def split(value):
    high = value.astype(BF16)
    return high, (value - high.astype(F32)).astype(BF16)


def middle_kernel(states_here, ids_ref, stats_ref, here_ref, target_ref, keep_ref, came_ref, h_ref, bo_ref, bp_ref, extra_ref, log_ref, grad_ref):
    rows, half = keep_ref.shape
    peaks = stats_ref[:, 0, :]
    peak = jnp.max(peaks, 0, keepdims=True)
    mass = jnp.sum(stats_ref[:, 1, :] * jnp.exp(peaks - peak), 0, keepdims=True)
    lane = lax.broadcasted_iota(jnp.int32, (1, 128), 1)
    log_partition = jnp.where(lane < states_here, peak + jnp.log(jnp.where(lane < states_here, mass, 1.0)), 0.0)
    log_ref[...] = log_partition[:, :states_here]
    at = lax.broadcasted_iota(jnp.int32, (8, 128), 0)
    pair = jnp.where(at == 0, log_partition, 0.0)
    state = lax.broadcasted_iota(jnp.int32, (128, rows), 0)
    row = lax.broadcasted_iota(jnp.int32, (128, rows), 1)
    spread = ((row >> 3) == state).astype(F32)
    pair = jnp.dot(pair, spread, precision=lax.Precision.HIGHEST, preferred_element_type=F32)
    log_rows = pair[0:1]
    goals = jnp.broadcast_to(target_ref[...], (8, states_here))
    target_rows = jnp.dot(goals, spread[:states_here], precision=lax.Precision.HIGHEST, preferred_element_type=F32)[0:1]
    member = ids_ref[0] * 8 + ids_ref[1] * 2 + ids_ref[2]
    lead = (lax.broadcasted_iota(jnp.int32, (1, rows), 1) & 7) == 0

    def graded(score, flag):
        is_data = jnp.logical_and(lead, jnp.broadcast_to(flag, lead.shape))
        gap = score - target_rows
        grad = penalty_weight * jnp.exp(score - log_rows)
        grad = grad + jnp.where(is_data, gap - penalty_weight, 0.0)
        loss = jnp.where(is_data, penalty_weight * (log_rows - score) + 0.5 * gap * gap, 0.0)
        return grad, loss

    grad_here, loss = graded(here_ref[...], member == 0)
    partner = ids_ref[0] * 8 + ids_ref[1] * 2 + 1 - ids_ref[2]
    sent = stats_ref[partner]
    there = jnp.concatenate([sent[k + 2 : k + 3] for k in range(rows // 128)], 1)
    grad_there, _ = graded(there, member + 1 - 2 * ids_ref[2] == 0)
    at = lax.broadcasted_iota(jnp.int32, (8, rows), 0)
    grads = jnp.where(at == 0, grad_here, grad_there)
    grad_ref[...] = grads.T
    loss = jnp.sum(loss, 1, keepdims=True)

    def scaled(i, carry):
        r = pl.ds(pl.multiple_of(i * 64, 64), 64)
        bo_ref[r, :] = (keep_ref[r, :].astype(F32) * grad_ref[r, 0:1]).astype(BF16)
        bp_ref[r, :] = (came_ref[r, :].astype(F32) * grad_ref[r, 1:2]).astype(BF16)
        return carry

    lax.fori_loop(0, rows // 64, scaled, 0, unroll=4)
    high, low = split(grad_here)
    weights = jnp.where(at == 0, high.astype(F32), low.astype(F32))
    weights = jnp.where(at < 2, weights, 0.0).astype(BF16)
    head = jnp.dot(weights, h_ref[...], preferred_element_type=F32)
    head = head[0:1] + head[1:2]
    pack_extra(extra_ref, [head[:, :half], head[:, half:], jnp.broadcast_to(loss, (1, half))])


def pack_extra(ref, parts):
    at = lax.broadcasted_iota(jnp.int32, ref.shape, 0)
    out = jnp.zeros(ref.shape, F32)
    for i, part in enumerate(parts):
        high, low = split(part)
        out = jnp.where(at == i, high.astype(F32), out)
        out = jnp.where(at == i + 8, low.astype(F32), out)
    ref[...] = out.astype(BF16)


def middle(ids, stats, here, targets, keep, came, h, states_here):
    rows, half = keep.shape
    whole = pl.BlockSpec(memory_space=pltpu.VMEM)
    return pl.pallas_call(
        functools.partial(middle_kernel, states_here),
        in_specs=[pl.BlockSpec(memory_space=pltpu.SMEM)] + [whole] * 6,
        out_specs=[whole] * 4,
        out_shape=[
            jax.ShapeDtypeStruct((rows, half), BF16),
            jax.ShapeDtypeStruct((rows, half), BF16),
            jax.ShapeDtypeStruct((16, half), BF16),
            jax.ShapeDtypeStruct((1, states_here), F32),
        ],
        scratch_shapes=[pltpu.VMEM((rows, 8), F32)],
        compiler_params=pltpu.CompilerParams(vmem_limit_bytes=6 << 20),
        cost_estimate=pl.CostEstimate(flops=1 << 30, bytes_accessed=9 << 20, transcendentals=0),
        name="middle",
    )(ids, stats, here, targets, keep, came, h)


def ways(ids_ref):
    x, y, core = ids_ref[0], ids_ref[1], ids_ref[2]
    return jnp.where(core == 0, x, y), jnp.where(core == 0, y, x), core


def gradient_kernel(turn, sides, relayed, ids_ref, xo_ref, xp_ref, bo_ref, bp_ref, extra_ref, *refs):
    near, _, core = ways(ids_ref)
    at = lax.rem(near + turn, 4)
    base = at * jnp.where(core == 0, 64, 16)
    stride = jnp.where(core == 0, 16, 64)
    outs = refs[1:] if relayed else refs
    count, cols = xo_ref.shape[0] // 4, outs[0].shape[1]

    def rows(ref):
        starts = [pl.multiple_of(z * 256 + base + i * stride, 16) for z in range(8) for i in range(4)]
        return jnp.concatenate([ref[pl.ds(start, 16), :] for start in starts], 0)

    here, there = rows(xo_ref), rows(xp_ref)
    for side, out_ref in zip(sides, outs):
        part = slice(side * cols, side * cols + cols)
        total = jnp.dot(here, bo_ref[:, part], preferred_element_type=F32)
        total += jnp.dot(there, bp_ref[:, part], preferred_element_type=F32)
        if relayed:
            total += refs[0][:count, :].astype(F32)
            out_ref[count + 16 : count + 32, :] = refs[0][count : count + 16, :]
        out_ref[:count, :] = total.astype(BF16)
        out_ref[count : count + 16, :] = extra_ref[:, part]


def gradient(turn, sides, relay, ids, xo, xp, bo, bp, extra):
    width, depth = xo.shape
    cols = bo.shape[1] // 2
    count = width // 4
    whole = pl.BlockSpec(memory_space=pltpu.VMEM)
    height = count + (16 if relay is None else 32)
    relays = () if relay is None else (relay,)
    return pl.pallas_call(
        functools.partial(gradient_kernel, turn, sides, relay is not None),
        in_specs=[pl.BlockSpec(memory_space=pltpu.SMEM)] + [whole] * (5 + len(relays)),
        out_specs=[whole] * len(sides),
        out_shape=[jax.ShapeDtypeStruct((height, cols), BF16)] * len(sides),
        compiler_params=pltpu.CompilerParams(vmem_limit_bytes=12 << 20),
        cost_estimate=pl.CostEstimate(flops=4 * count * cols * len(sides) * depth, bytes_accessed=4 << 20, transcendentals=0),
        name="gradient",
    )(ids, xo, xp, bo, bp, extra, *relays)


def ordered_extra(scratch_ref, order, values):
    for k, value in enumerate(values):
        scratch_ref[order[k]] = value
    total = scratch_ref[0]
    for k in range(1, len(values)):
        total = total + scratch_ref[k]
    return total


def fold_kernel(ids_ref, *refs):
    own, plus, minus, outs, scratch_ref = refs[0:2], refs[2:4], refs[4:6], refs[6:10], refs[10]
    near, far, _ = ways(ids_ref)
    cols = own[0].shape[1]
    for k in (1, 2, 3, 0):
        spot = lax.rem(far + k, 4) * 16
        for z in range(8):
            r = pl.ds(pl.multiple_of(z * 64 + spot, 16), 16)
            for side in range(2):
                value = own[side][r, :].astype(F32) + plus[side][r, :].astype(F32) + minus[side][r, :].astype(F32)
                outs[k][z * 16 : z * 16 + 16, side * cols : side * cols + cols] = value.astype(outs[k].dtype)
    first, second = slice(512, 528), slice(528, 544)
    sets = [
        (own[0][first, :], own[1][first, :]),
        (plus[0][first, :], plus[1][first, :]),
        (plus[0][second, :], minus[1][second, :]),
        (minus[0][first, :], minus[1][first, :]),
    ]
    whole = [jnp.concatenate([left.astype(F32), right.astype(F32)], 1) for left, right in sets]
    total = ordered_extra(scratch_ref, [lax.rem(near + k, 4) for k in (0, 3, 2, 1)], [v[:8] + v[8:] for v in whole])
    high, low = split(total)
    block = jnp.concatenate([high.astype(F32), low.astype(F32)], 0)
    for k in range(4):
        outs[k][128:144, :] = block.astype(outs[k].dtype)


def fold(ids, own, plus, minus):
    whole = pl.BlockSpec(memory_space=pltpu.VMEM)
    cols = 2 * own[0].shape[1]
    return pl.pallas_call(
        fold_kernel,
        in_specs=[pl.BlockSpec(memory_space=pltpu.SMEM)] + [whole] * 6,
        out_specs=[whole] * 4,
        out_shape=[jax.ShapeDtypeStruct((144, cols), F32 if k == 0 else BF16) for k in range(4)],
        scratch_shapes=[pltpu.VMEM((4, 8, cols), F32)],
        compiler_params=pltpu.CompilerParams(vmem_limit_bytes=6 << 20),
        cost_estimate=pl.CostEstimate(flops=1 << 20, bytes_accessed=3 << 20, transcendentals=0),
        name="fold",
    )(ids, *own, *plus, *minus)


def join_kernel(ids_ref, *refs):
    got, out_ref, scratch_ref = refs[0:4], refs[4], refs[5]
    half = got[0].shape[1]
    _, far, _ = ways(ids_ref)
    whole = [ref[128:144, :].astype(F32) for ref in got]
    total = ordered_extra(scratch_ref, [lax.rem(far + k, 4) for k in (0, 3, 2, 1)], [v[:8] + v[8:] for v in whole])
    pieces = [total[i : i + 1, j * 128 : (j + 1) * 128] for i in range(2) for j in range(half // 128)]
    pieces += [part.astype(F32) for part in split(total[2:3, :128])]
    at = lax.broadcasted_iota(jnp.int32, (16, 128), 0)
    tail = []
    for group in (pieces[:16], pieces[16:]):
        block = jnp.zeros((16, 128), F32)
        for i, piece in enumerate(group):
            block = jnp.where(at == i, piece, block)
        tail.append(block)
    tail = jnp.concatenate(tail, 1).astype(BF16)
    for i in range(8):
        out_ref[i, :, :half] = sum(ref[i * 16 : i * 16 + 16, :].astype(F32) for ref in got).astype(BF16)
        out_ref[i, :, half:] = tail


def join(ids, got):
    whole = pl.BlockSpec(memory_space=pltpu.VMEM)
    half = got[0].shape[1]
    return pl.pallas_call(
        join_kernel,
        in_specs=[pl.BlockSpec(memory_space=pltpu.SMEM)] + [whole] * 4,
        out_specs=whole,
        out_shape=jax.ShapeDtypeStruct((8, 16, half + 256), BF16),
        scratch_shapes=[pltpu.VMEM((4, 8, half), F32)],
        compiler_params=pltpu.CompilerParams(vmem_limit_bytes=4 << 20),
        cost_estimate=pl.CostEstimate(flops=1 << 20, bytes_accessed=2 << 20, transcendentals=0),
        name="join",
    )(ids, *got)


def near_kernel(ids_ref, all_ref, mine_ref, other_ref):
    half = mine_ref.shape[1]
    total = all_ref[0].astype(F32)
    for z in range(1, all_ref.shape[0]):
        total += all_ref[z].astype(F32)
    top, low = total[:8], total[8:]
    lead = jnp.broadcast_to(ids_ref[2] == 0, (8, half))
    mine_ref[0:8, :] = jnp.where(lead, top[:, :half], low[:, :half])
    other_ref[0:8, :] = jnp.where(lead, low[:, :half], top[:, :half])
    extra = jnp.concatenate([top[:, half:], low[:, half:]], 1)
    for ref in (mine_ref, other_ref):
        ref[8:16, :] = jnp.zeros((8, half), F32)
        ref[8:16, 0:512] = extra


def near(ids, everything):
    whole = pl.BlockSpec(memory_space=pltpu.VMEM)
    half = everything.shape[2] - 256
    return pl.pallas_call(
        near_kernel,
        in_specs=[pl.BlockSpec(memory_space=pltpu.SMEM), whole],
        out_specs=[whole] * 2,
        out_shape=[jax.ShapeDtypeStruct((16, half), F32)] * 2,
        compiler_params=pltpu.CompilerParams(vmem_limit_bytes=4 << 20),
        cost_estimate=pl.CostEstimate(flops=1 << 20, bytes_accessed=1 << 20, transcendentals=0),
        name="near",
    )(ids, everything)


def last_kernel(scale, ids_ref, mine_ref, came_ref, hidden_ref, head_ref, loss_ref):
    half = hidden_ref.shape[1] // 2
    mine, came = mine_ref[0:8, :], came_ref[0:8, :]
    lead = jnp.broadcast_to(ids_ref[2] == 0, mine.shape)
    hidden_ref[:, :half] = jnp.where(lead, mine, came)
    hidden_ref[:, half:] = jnp.where(lead, came, mine)
    total = mine_ref[8:16, 0:512] + came_ref[8:16, 0:512]
    head_ref[0:8, :] = total[:, 0:128]
    head_ref[8:16, :] = total[:, 256:384]
    loss_ref[...] = (total[0:1, 128:256] + total[1:2, 128:256]) * scale


def last(ids, mine, came, states_total):
    whole = pl.BlockSpec(memory_space=pltpu.VMEM)
    width = 2 * mine.shape[1]
    return pl.pallas_call(
        functools.partial(last_kernel, 1.0 / states_total),
        in_specs=[pl.BlockSpec(memory_space=pltpu.SMEM), whole, whole],
        out_specs=[whole] * 3,
        out_shape=[
            jax.ShapeDtypeStruct((8, width), F32),
            jax.ShapeDtypeStruct((16, 128), F32),
            jax.ShapeDtypeStruct((1, 128), F32),
        ],
        compiler_params=pltpu.CompilerParams(vmem_limit_bytes=4 << 20),
        name="last",
    )(ids, mine, came)


def gathered(state_features, ids):
    own = jnp.where(jnp.sum(ids) < 0, jnp.zeros_like(state_features), state_features)
    own = jnp.broadcast_to(own.T, (16, *state_features.shape[::-1]))
    mine = lax.all_to_all(own, ("x", "y"), split_axis=0, concat_axis=0, tiled=True)
    return mine, shifted(mine, "c", 1)


def step(state_features, action_features, targets, w_hidden, w_head):
    states_here, actions_here, width = action_features.shape
    states_total = states_here * lax.axis_size("z")
    rows = states_here * actions_here
    ids = jnp.stack([lax.axis_index(axis) for axis in (*ACT, "z")]).astype(jnp.int32)
    members = lax.axis_size(ACT)
    mine, other = gathered(state_features, ids)
    xt, keep, send, h, score, stats = forward(
        ids, mine, other, action_features.reshape(rows, width), w_hidden, w_head[None], members
    )
    stats = lax.all_to_all(stats, ACT, split_axis=0, concat_axis=0, tiled=True)
    came = shifted(send, "c", 1)
    xt_there = shifted(xt, "c", 1)
    b_here, b_there, extra, log_row = middle(ids, stats, score, targets[None], keep, came, h, states_here)

    def piece(turn, sides, relay=None):
        return gradient(turn, sides, relay, ids, xt, xt_there, b_here, b_there, extra)

    def turned(value, k, swap):
        pairs = []
        for i in range(32):
            px, py, pc = i // 8, i // 2 % 4, i % 2
            along_x = (pc == 0) != swap
            to = (px + k) % 4 * 8 + py * 2 + pc if along_x else px * 8 + (py + k) % 4 * 2 + pc
            pairs.append((i, to))
        return lax.ppermute(value, ACT, pairs)

    def sent(value, k):
        return turned(value, k, False)

    far_left, far_right = piece(2, (0, 1))
    relay_left = sent(far_left, 1)
    relay_right = sent(far_right, 3)
    plus_right = sent(piece(1, (1,))[0], 1)
    minus_left = sent(piece(3, (0,))[0], 3)
    own = piece(0, (0, 1))
    plus_left = sent(piece(1, (0,), relay_left)[0], 1)
    minus_right = sent(piece(3, (1,), relay_right)[0], 3)
    folded = fold(ids, own, (plus_left, plus_right), (minus_left, minus_right))
    more = [folded[0]]
    for k in (1, 2, 3):
        more.append(turned(folded[k], k, True))
    joined = join(ids, more)
    everything = lax.all_to_all(joined, "z", split_axis=0, concat_axis=0, tiled=True)
    mine, away = near(ids, everything)
    came = shifted(away, "c", 1)
    hidden, head, loss = last(ids, mine, came, states_total)
    return (hidden, head.reshape(-1), log_row.reshape(states_here), loss[0, 0])


def solution(mesh):
    finer = Mesh(mesh.devices.reshape(mesh.shape["state"], 4, 4, 2), EVERY)
    placed = (P("z", ACT), P("z", ACT, None), P("z"), P(), P())
    return jax.shard_map(
        step,
        mesh=finer,
        in_specs=placed,
        out_specs=(P(EVERY, None), P(), P("z"), P()),
        check_vma=False,
    )
```
